256 devices in a mesh: dp: 8 (over x, core), fsdp: 8 (over z), mp: 4 (over y).
Axes of the slice: x: 4, y: 4, z: 8, core: 2. Of those that a mesh axis runs over, the one named last changes fastest.
Arguments:
- gradients: bfloat16 [64, 12, 2, 256, 1024], P(('dp', 'fsdp'), None, None, None, 'mp'), may hold values from -16 to 16
- master: float32 [12, 2, 256, 1024], P(None, None, ('dp', 'fsdp'), 'mp'), may hold values from -0.375 to 0.375
- teacher: float32 [12, 2, 256, 1024], P(None, None, ('dp', 'fsdp'), 'mp'), may hold values from -0.375 to 0.375
- first_moment: float32 [12, 2, 256, 1024], P(None, None, ('dp', 'fsdp'), 'mp'), may hold values from -2.2888184e-05 to 2.2888184e-05
- second_moment: float32 [12, 2, 256, 1024], P(None, None, ('dp', 'fsdp'), 'mp'), may hold values from 0 to 1, as said below
- layer_rates: float32 [12], replicated, may hold values from 0.02 to 0.2
Outputs:
- master_new: float32 [12, 2, 256, 1024], P(None, None, ('dp', 'fsdp'), 'mp')
- teacher_new: float32 [12, 2, 256, 1024], P(None, None, ('dp', 'fsdp'), 'mp')
- first_new: float32 [12, 2, 256, 1024], P(None, None, ('dp', 'fsdp'), 'mp')
- second_new: float32 [12, 2, 256, 1024], P(None, None, ('dp', 'fsdp'), 'mp')
- student_weights: bfloat16 [12, 2, 256, 1024], P(None, None, None, 'mp')
- teacher_weights: bfloat16 [12, 2, 256, 1024], P(None, None, None, 'mp')
The draws below stay inside these ranges and needn't reach their ends.
Inputs may be any that keep to these rules, and one draw needn't show every extreme that they name: `second_moment`: every entry is positive.
All inputs are finite; a program needn't handle non-finite values.
Results may differ from the reference program's by a relative error of at most 0.0004.
Values may be sent and summed in bfloat16 or wider, within the bound.
No kernel may reach another device: no remote copies, remote signals or barrier semaphores. Data moves between devices by JAX's collectives and lax.ppermute only.
A program may use at most 64 MiB of HBM per device.

```python
import math
import jax
import jax.numpy as jnp
from jax import lax

D = 256
FF = 1024
LAYERS = 12
NDATA = 64


def draw_second_moment(key, part):
    typical = 0.01 / (2.0 * LAYERS * D * FF)
    spread = jax.random.uniform(key, (LAYERS, 2, D, FF), jnp.float32, -2.3, 2.3)
    return typical * jnp.exp(spread)


def spiked(entries, rng, source, target, blocks, factor):
    def block_of(axis_at):
        return (jnp.arange(entries.shape[axis_at]) // (entries.shape[axis_at] // blocks)).reshape((-1,) + (1,) * (entries.ndim - 1 - axis_at))

    first = jax.random.permutation(rng, blocks)[block_of(target)]
    other_side = (block_of(target) + blocks // 2) % blocks
    return jnp.where((block_of(source) == first) | (block_of(source) == other_side), factor * entries, entries)


def level_of(rng, extent, pieces, low, largest):
    factor_of, own = 1.0, jax.random.fold_in(rng, 6)
    for dim, parts in pieces:
        heights = jnp.exp(jax.random.uniform(jax.random.fold_in(own, dim), (parts,), jnp.float32, low / len(pieces), largest / len(pieces)))
        factor_of = factor_of * jnp.repeat(heights, extent[dim] // parts).reshape([-1 if axis == dim else 1 for axis in range(len(extent))])
    return factor_of


def noise(key, extent, width, reach, pieces=(), held_as=jnp.bfloat16):
    drawn = width * jax.random.normal(key, extent, jnp.float32)
    if pieces:
        drawn = drawn * level_of(key, extent, pieces, -0.22, 0.18)
    return jnp.clip(drawn, -reach, reach).astype(held_as)


def gaussian_with(own_key, shape, deviation, reach, split, heavy, dtype=jnp.bfloat16):
    drawn = deviation * jax.random.normal(own_key, shape, jnp.float32)
    if split:
        drawn = drawn * level_of(own_key, shape, split, -0.22, 0.18)
    return jnp.clip(spiked(drawn, jax.random.fold_in(own_key, 3), *heavy), -reach, reach).astype(dtype)


def setup_inputs(seed: int = 0) -> dict:
    keys = jax.random.split(jax.random.key(seed), 7)
    gradients = gaussian_with(keys[0], (NDATA, LAYERS, 2, D, FF), 1.0, 16.0, ((0, 64), (4, 4)), (0, 3, 64, 4.0))
    master = noise(keys[1], (LAYERS, 2, D, FF), D ** -0.5, 0.375, ((2, 64), (3, 4)), jnp.float32)
    teacher = noise(keys[2], (LAYERS, 2, D, FF), D ** -0.5, 0.375, ((2, 64), (3, 4)), jnp.float32)
    first_moment = noise(keys[3], (LAYERS, 2, D, FF), (20000 * LAYERS * D * FF) ** -0.5, 2.288818359375e-05, ((2, 64), (3, 4)), jnp.float32)
    second_moment = draw_second_moment(jax.random.fold_in(keys[6], 71), 0)
    layer_rates = jnp.clip(jnp.exp(jax.random.uniform(keys[5], (LAYERS,), jnp.float32, math.log(0.02), math.log(0.2))), 0.02, 0.2)
    return {"gradients": gradients, "master": master, "teacher": teacher, "first_moment": first_moment, "second_moment": second_moment, "layer_rates": layer_rates}


CLIP_NORM = 0.1
BETA_ONE = 0.9
BETA_TWO = 0.999
BIAS_ONE = 1.0 - 0.9 ** 50 * 0.9 ** 50
BIAS_TWO = 1.0 - 0.999 ** 50 * 0.999 ** 50
ADAM_EPS = 1e-08
DECAY = 0.05
EMA_KEEP = 0.95

def accumulate(carry, piece):
    return (carry + piece.astype(jnp.float32), jnp.zeros((), jnp.float32))

def reference(gradients, master, teacher, first_moment, second_moment, layer_rates):
    summed, unused = lax.scan(accumulate, jnp.zeros(gradients.shape[1:], jnp.float32), gradients)
    mean_grad = summed / gradients.shape[0]
    norm_sq = jnp.sum(mean_grad * mean_grad)
    clip_factor = jnp.minimum(1.0, CLIP_NORM / (jnp.sqrt(norm_sq) + 1e-06))
    clipped = clip_factor * mean_grad
    first_new = BETA_ONE * first_moment + (1.0 - BETA_ONE) * clipped
    second_new = BETA_TWO * second_moment + (1.0 - BETA_TWO) * clipped * clipped
    direction = first_new / BIAS_ONE / (jnp.sqrt(second_new / BIAS_TWO) + ADAM_EPS) + DECAY * master
    layer_rate = layer_rates[:, None, None, None]
    master_new = master - layer_rate * direction
    teacher_new = EMA_KEEP * teacher + (1.0 - EMA_KEEP) * master_new
    return (master_new, teacher_new, first_new, second_new, master_new.astype(jnp.bfloat16), teacher_new.astype(jnp.bfloat16))
```

```python
import jax
import jax.numpy as jnp
from jax import lax
from jax.sharding import PartitionSpec as P

OWN = ("dp", "fsdp")
ALL = ("dp", "fsdp", "mp")

CLIP_NORM = 0.1
BETA_ONE = 0.9
BETA_TWO = 0.999
BIAS_ONE = 1.0 - 0.9**50 * 0.9**50
BIAS_TWO = 1.0 - 0.999**50 * 0.999**50
ADAM_EPS = 1e-08
DECAY = 0.05
EMA_KEEP = 0.95


def shards(gradients, master, teacher, first_moment, second_moment, layer_rates):
    own_grad = gradients[0].astype(jnp.float32)
    summed = lax.psum_scatter(own_grad, OWN, scatter_dimension=2, tiled=True)
    mean_grad = summed / 64.0
    norm_sq = lax.psum(jnp.sum(mean_grad * mean_grad), ALL)
    clip_factor = jnp.minimum(1.0, CLIP_NORM / (jnp.sqrt(norm_sq) + 1e-06))
    clipped = clip_factor * mean_grad
    first_new = BETA_ONE * first_moment + (1.0 - BETA_ONE) * clipped
    second_new = BETA_TWO * second_moment + (1.0 - BETA_TWO) * clipped * clipped
    direction = first_new / BIAS_ONE / (jnp.sqrt(second_new / BIAS_TWO) + ADAM_EPS) + DECAY * master
    layer_rate = layer_rates[:, None, None, None]
    master_new = master - layer_rate * direction
    teacher_new = EMA_KEEP * teacher + (1.0 - EMA_KEEP) * master_new
    student = lax.all_gather(master_new.astype(jnp.bfloat16), OWN, axis=2, tiled=True)
    teach = lax.all_gather(teacher_new.astype(jnp.bfloat16), OWN, axis=2, tiled=True)
    return (master_new, teacher_new, first_new, second_new, student, teach)


def solution(mesh):
    own = P(None, None, OWN, "mp")
    gathered = P(None, None, None, "mp")
    in_specs = (P(OWN, None, None, None, "mp"), own, own, own, own, P())
    out_specs = (own, own, own, own, gathered, gathered)
    return jax.shard_map(shards, mesh=mesh, in_specs=in_specs, out_specs=out_specs, check_vma=False)
```

```python
import jax
import jax.numpy as jnp
from jax import lax
from jax.experimental import pallas as pl
from jax.experimental.pallas import tpu as pltpu
from jax.sharding import Mesh
from jax.sharding import PartitionSpec as P


OWN = ("x", "c", "z")
ALL = ("x", "c", "z", "y")

CLIP_NORM = 0.1
BETA_ONE = 0.9
BETA_TWO = 0.999
BIAS_ONE = 1.0 - 0.9**50 * 0.9**50
BIAS_TWO = 1.0 - 0.999**50 * 0.999**50
ADAM_EPS = 1e-08
DECAY = 0.05
EMA_KEEP = 0.95

F32 = jnp.float32
BF16 = jnp.bfloat16


def shift(v, axis, by):
    n = lax.axis_size(axis)
    return lax.ppermute(v, axis, [(i, (i + by) % n) for i in range(n)])


def pick(v, index, axis):
    return lax.dynamic_index_in_dim(v, index, axis, keepdims=False)


def scatter_x(part):
    half = part[0].shape[0] // 2
    far_r, far_l = part[2][:half], part[2][half:]
    got_r = shift(far_r, "x", 1)
    got_l = shift(far_l, "x", -1)
    easy_r = shift(part[1][half:], "x", 1)
    easy_l = shift(part[3][:half], "x", -1)
    last_r = shift(part[1][:half] + got_r, "x", 1)
    last_l = shift(part[3][half:] + got_l, "x", -1)
    low = part[0][:half] + easy_l + last_r
    high = part[0][half:] + easy_r + last_l
    return jnp.concatenate([low, high], axis=0)


def scatter_z(part):
    half = part[0].shape[0] // 2
    r = shift(part[4][:half], "z", 1)
    l = shift(part[4][half:], "z", -1)
    r = jnp.concatenate([part[3][:half] + r, part[3][half:]], axis=0)
    l = jnp.concatenate([part[5][:half], part[5][half:] + l], axis=0)
    for j in (2, 1, 0):
        r = part[j] + shift(r, "z", 1) if j else shift(r, "z", 1)
        l = part[8 - j] + shift(l, "z", -1) if j else shift(l, "z", -1)
    return part[0] + r + l


def gather_z(u):
    half = u.shape[0] // 2
    v = [u] + [None] * 7
    r, l = u, u
    for j in (1, 2, 3):
        r = shift(r, "z", 1)
        l = shift(l, "z", -1)
        v[8 - j], v[j] = r, l
    v[4] = jnp.concatenate([shift(r[:half], "z", 1), shift(l[half:], "z", -1)], axis=0)
    return v


def gather_x(s, t):
    s_l = shift(s, "x", 1)
    t_r = shift(t, "x", -1)
    t_l = shift(t, "x", 1)
    s_r = shift(s, "x", -1)
    s_far = shift(s_l, "x", 1)
    t_far = shift(t_r, "x", -1)
    return [s, s_r, s_far, s_l], [t, t_r, t_far, t_l]


def place(mine, other, at_x, at_c):
    def kernel(where, *refs):
        src, out, sems = refs[:8], refs[8], refs[9]
        copies = []
        for j in range(4):
            for k in range(2):
                row = where[0] + j
                row = jnp.where(row >= 4, row - 4, row)
                core = where[1] if k == 0 else 1 - where[1]
                copies.append(
                    pltpu.make_async_copy(src[4 * k + j], out.at[:, row * 2 + core], sems.at[4 * k + j])
                )
        for copy in copies:
            copy.start()
        for copy in copies:
            copy.wait()

    anywhere = pl.BlockSpec(memory_space=pl.ANY)
    out = pl.pallas_call(
        kernel,
        out_shape=jax.ShapeDtypeStruct((24, 8, 32, 256), BF16),
        in_specs=[pl.BlockSpec(memory_space=pltpu.SMEM)] + [anywhere] * 8,
        out_specs=anywhere,
        scratch_shapes=[pltpu.SemaphoreType.DMA((8,))],
        name="place",
    )(jnp.stack([at_x, at_c]), *mine, *other)
    return out.reshape(12, 2, 256, 256)


def total(value):
    spread = jnp.broadcast_to(value, (256, 128))
    return jnp.sum(lax.all_to_all(spread, ALL, 0, 0, tiled=True)[:, 0])


def shards(gradients, master, teacher, first_moment, second_moment, layer_rates):
    x, c, z = lax.axis_index("x"), lax.axis_index("c"), lax.axis_index("z")
    own = gradients.reshape(24, 4, 2, 32, 256)
    keep, give = pick(own, c, 2), pick(own, 1 - c, 2)
    part = [None] * 4
    for j in (2, 1, 3, 0):
        at = (x + j) % 4
        got = shift(pick(give, at, 1), "c", 1)
        part[j] = pick(keep, at, 1).astype(F32) + got.astype(F32)
    over_x = scatter_x(part).reshape(24, 8, 4, 256).transpose(1, 0, 2, 3)
    summed = scatter_z([pick(over_x, (z + j) % 8, 0) for j in range(8)])
    mean_grad = summed.reshape(12, 2, 4, 256) / 64.0
    norm_sq = total(jnp.sum(mean_grad * mean_grad))
    clip_factor = jnp.minimum(1.0, CLIP_NORM / (jnp.sqrt(norm_sq) + 1e-06))
    clipped = clip_factor * mean_grad
    first_new = BETA_ONE * first_moment + (1.0 - BETA_ONE) * clipped
    second_new = BETA_TWO * second_moment + (1.0 - BETA_TWO) * clipped * clipped
    direction = first_new / BIAS_ONE / (jnp.sqrt(second_new / BIAS_TWO) + ADAM_EPS) + DECAY * master
    layer_rate = layer_rates[:, None, None, None]
    master_new = master - layer_rate * direction
    teacher_new = EMA_KEEP * teacher + (1.0 - EMA_KEEP) * master_new
    both = jnp.concatenate([master_new.astype(BF16), teacher_new.astype(BF16)], axis=0).reshape(48, 4, 256)
    pieces = jnp.stack(gather_z(both))
    pieces = lax.dynamic_slice_in_dim(jnp.concatenate([pieces, pieces], axis=0), (8 - z) % 8, 8, axis=0)
    pieces = pieces.transpose(1, 0, 2, 3).reshape(48, 32, 256)
    students, teachers = gather_x(pieces[:24], pieces[24:])
    other_students = [shift(s, "c", 1) for s in students]
    other_teachers = [shift(t, "c", 1) for t in teachers]
    student = place(students, other_students, x, c)
    teach = place(teachers, other_teachers, x, c)
    return (master_new, teacher_new, first_new, second_new, student, teach)


def solution(mesh):
    torus = Mesh(mesh.devices.reshape(4, 2, 8, 4), ("x", "c", "z", "y"))
    own = P(None, None, OWN, "y")
    gathered = P(None, None, None, "y")
    in_specs = (P(OWN, None, None, None, "y"), own, own, own, own, P())
    out_specs = (own, own, own, own, gathered, gathered)
    return jax.shard_map(shards, mesh=torus, in_specs=in_specs, out_specs=out_specs, check_vma=False)
```

```python
import jax
import jax.numpy as jnp
from jax import lax
from jax.sharding import Mesh
from jax.sharding import PartitionSpec as P


OWN = ("x", "c", "z")
ALL = ("x", "c", "z", "y")

CLIP_NORM = 0.1
BETA_ONE = 0.9
BETA_TWO = 0.999
BIAS_ONE = 1.0 - 0.9**50 * 0.9**50
BIAS_TWO = 1.0 - 0.999**50 * 0.999**50
ADAM_EPS = 1e-08
DECAY = 0.05
EMA_KEEP = 0.95

F32 = jnp.float32
BF16 = jnp.bfloat16


def shift(v, axis, by):
    n = lax.axis_size(axis)
    return lax.ppermute(v, axis, [(i, (i + by) % n) for i in range(n)])


def pick(v, index, axis):
    return lax.dynamic_index_in_dim(v, index, axis, keepdims=False)


def scatter_z(part, half):
    near, far = (1, -1) if half == 0 else (-1, 1)
    long = shift(part[4], "z", near)
    for j in (3, 2, 1):
        long = shift(part[4 + near * (j - 4)] + long, "z", near)
    short = shift(part[4 + near], "z", far)
    for j in (2, 1):
        short = shift(part[(8 + far * j) % 8] + short, "z", far)
    return part[0] + long + short


def gather_z(u):
    half = u.shape[0] // 2
    v = [u] + [None] * 7
    r, l = u, u
    for j in (1, 2, 3):
        r = shift(r, "z", 1)
        l = shift(l, "z", -1)
        v[8 - j], v[j] = r, l
    v[4] = jnp.concatenate([shift(r[:half], "z", 1), shift(l[half:], "z", -1)], axis=0)
    return v


def gather_x(s, t):
    s_l = shift(s, "x", 1)
    t_r = shift(t, "x", -1)
    t_l = shift(t, "x", 1)
    s_r = shift(s, "x", -1)
    s_far = shift(s_l, "x", 1)
    t_far = shift(t_r, "x", -1)
    return [s, s_r, s_far, s_l], [t, t_r, t_far, t_l]


def place(pieces, at):
    out = jnp.zeros((pieces[0].shape[0], len(pieces)) + pieces[0].shape[1:], pieces[0].dtype)
    for piece, index in zip(pieces, at):
        out = lax.dynamic_update_index_in_dim(out, piece, index, 1)
    return out


def total(value):
    spread = jnp.broadcast_to(value, (256, 128))
    return jnp.sum(lax.all_to_all(spread, ALL, 0, 0, tiled=True)[:, 0])


def shards(gradients, master, teacher, first_moment, second_moment, layer_rates):
    x, c, z = lax.axis_index("x"), lax.axis_index("c"), lax.axis_index("z")
    own = gradients.reshape(24, 4, 2, 32, 256)
    keep, give = pick(own, c, 2), pick(own, 1 - c, 2)
    halves = []
    got = [shift(give[:12], "c", 1), shift(give[12:], "c", 1)]
    for h in range(2):
        part = keep[12 * h : 12 * h + 12].astype(F32) + got[h].astype(F32)
        part = lax.optimization_barrier(part.reshape(12, 4, 8, 4, 256).transpose(2, 0, 1, 3, 4))
        halves.append(scatter_z([pick(part, (z + j) & 7, 0) for j in range(8)], h))
    over_z = jnp.concatenate(halves, axis=0).transpose(1, 0, 2, 3)
    summed = jnp.sum(lax.all_to_all(over_z, "x", 0, 0, tiled=True), axis=0)
    mean_grad = summed.reshape(12, 2, 4, 256) / 64.0
    norm_sq = total(jnp.sum(mean_grad * mean_grad))
    clip_factor = jnp.minimum(1.0, CLIP_NORM / (jnp.sqrt(norm_sq) + 1e-06))
    clipped = clip_factor * mean_grad
    first_new = BETA_ONE * first_moment + (1.0 - BETA_ONE) * clipped
    second_new = BETA_TWO * second_moment + (1.0 - BETA_TWO) * clipped * clipped
    direction = first_new / BIAS_ONE / (jnp.sqrt(second_new / BIAS_TWO) + ADAM_EPS) + DECAY * master
    layer_rate = layer_rates[:, None, None, None]
    master_new = master - layer_rate * direction
    teacher_new = EMA_KEEP * teacher + (1.0 - EMA_KEEP) * master_new
    both = jnp.concatenate([master_new.astype(BF16), teacher_new.astype(BF16)], axis=0).reshape(48, 4, 256)
    pieces = place(gather_z(both), [(z + j) & 7 for j in range(8)]).reshape(48, 32, 256)
    students, teachers = gather_x(pieces[:24], pieces[24:])
    at = [((x + j) & 3) * 2 for j in range(4)]
    at = [i + c for i in at] + [i + 1 - c for i in at]
    student = place(students + [shift(s, "c", 1) for s in students], at).reshape(12, 2, 256, 256)
    teach = place(teachers + [shift(t, "c", 1) for t in teachers], at).reshape(12, 2, 256, 256)
    return (master_new, teacher_new, first_new, second_new, student, teach)


def solution(mesh):
    torus = Mesh(mesh.devices.reshape(4, 2, 8, 4), ("x", "c", "z", "y"))
    own = P(None, None, OWN, "y")
    gathered = P(None, None, None, "y")
    in_specs = (P(OWN, None, None, None, "y"), own, own, own, own, P())
    out_specs = (own, own, own, own, gathered, gathered)
    return jax.shard_map(shards, mesh=torus, in_specs=in_specs, out_specs=out_specs, check_vma=False)
```

```python
import jax
import jax.numpy as jnp
from jax import lax
from jax.experimental import pallas as pl
from jax.experimental.pallas import tpu as pltpu
from jax.sharding import Mesh
from jax.sharding import PartitionSpec as P


OWN = ("x", "c", "z")
ALL = ("x", "c", "z", "y")

CLIP_NORM = 0.1
BETA_ONE = 0.9
BETA_TWO = 0.999
BIAS_ONE = 1.0 - 0.9**50 * 0.9**50
BIAS_TWO = 1.0 - 0.999**50 * 0.999**50
ADAM_EPS = 1e-08
DECAY = 0.05
EMA_KEEP = 0.95

F32 = jnp.float32
BF16 = jnp.bfloat16


def shift(v, axis, by):
    n = lax.axis_size(axis)
    return lax.ppermute(v, axis, [(i, (i + by) % n) for i in range(n)])


def pick(v, index, axis):
    return lax.dynamic_index_in_dim(v, index, axis, keepdims=False)


def chip_sum(own, got, c, half):
    def kernel(core, mine, other, out):
        both = mine[:, :, 0].astype(F32) + other[...].astype(F32)
        for z in range(8):
            out[z] = both[:, :, 4 * z : 4 * z + 4]

    step = 3
    return pl.pallas_call(
        kernel,
        out_shape=jax.ShapeDtypeStruct((8, 12, 4, 4, 256), F32),
        grid_spec=pltpu.PrefetchScalarGridSpec(
            num_scalar_prefetch=1,
            grid=(12 // step,),
            in_specs=[
                pl.BlockSpec((step, 4, 1, 32, 256), lambda i, core: (i + half * (12 // step), 0, core[0], 0, 0)),
                pl.BlockSpec((step, 4, 32, 256), lambda i, core: (i, 0, 0, 0)),
            ],
            out_specs=pl.BlockSpec((8, step, 4, 4, 256), lambda i, core: (0, i, 0, 0, 0)),
        ),
        name="chip_sum",
    )(c.reshape(1), own, got)


def pair(right, left, by, axis):
    right, left = lax.optimization_barrier((right, left))
    return shift(right, axis, by), shift(left, axis, -by)


def scatter_z(a, b):
    long_a, long_b = pair(a[4], b[4], 1, "z")
    short_b, short_a = pair(b[3], a[5], 1, "z")
    for j in (3, 2, 1):
        long_a, long_b = pair(a[j] + long_a, b[8 - j] + long_b, 1, "z")
        if j > 1:
            short_b, short_a = pair(b[j - 1] + short_b, a[9 - j] + short_a, 1, "z")
    return a[0] + long_a + short_a, b[0] + long_b + short_b


def scatter_x(part):
    right, left = pair(part[1], part[3], 1, "x")
    return part[0] + right + left + shift(part[2], "x", 2)


def gather_z(u):
    half = u.shape[0] // 2
    v = [u] + [None] * 7
    v[7], v[1] = shift(u, "z", 1), shift(u, "z", -1)
    v[6], v[2] = shift(u, "z", 2), shift(u, "z", -2)
    right = jnp.concatenate([v[7], v[6][:half]], axis=0)
    left = jnp.concatenate([v[1], v[2][half:]], axis=0)
    right, left = pair(right, left, 2, "z")
    v[5], v[3] = right[: 2 * half], left[: 2 * half]
    v[4] = jnp.concatenate([right[2 * half :], left[2 * half :]], axis=0)
    return v


def gather_x(s, t):
    s_l = shift(s, "x", 1)
    t_r = shift(t, "x", -1)
    t_l = shift(t, "x", 1)
    s_r = shift(s, "x", -1)
    s_far = shift(s_l, "x", 1)
    t_far = shift(t_r, "x", -1)
    return [s, s_r, s_far, s_l], [t, t_r, t_far, t_l]


def place(pieces, at):
    out = jnp.zeros((pieces[0].shape[0], len(pieces)) + pieces[0].shape[1:], pieces[0].dtype)
    for piece, index in zip(pieces, at):
        out = lax.dynamic_update_index_in_dim(out, piece, index, 1)
    return out


def total(value):
    spread = jnp.broadcast_to(value, (256, 128))
    return jnp.sum(lax.all_to_all(spread, ALL, 0, 0, tiled=True)[:, 0])


def shards(gradients, master, teacher, first_moment, second_moment, layer_rates):
    x, c, z = lax.axis_index("x"), lax.axis_index("c"), lax.axis_index("z")
    own = gradients.reshape(24, 4, 2, 32, 256)
    give = pick(own, 1 - c, 2)
    got = [shift(give[:12], "c", 1), shift(give[12:], "c", 1)]
    parts = [chip_sum(own, got[h], c, h) for h in range(2)]
    halves = [[pick(part, (z + j) & 7, 0) for j in range(8)] for part in parts]
    over_z = scatter_z(*halves)
    summed = scatter_x([jnp.concatenate([pick(v, (x + j) & 3, 1) for v in over_z], axis=0) for j in range(4)])
    mean_grad = summed.reshape(12, 2, 4, 256) / 64.0
    norm_sq = total(jnp.sum(mean_grad * mean_grad))
    clip_factor = jnp.minimum(1.0, CLIP_NORM / (jnp.sqrt(norm_sq) + 1e-06))
    clipped = clip_factor * mean_grad
    first_new = BETA_ONE * first_moment + (1.0 - BETA_ONE) * clipped
    second_new = BETA_TWO * second_moment + (1.0 - BETA_TWO) * clipped * clipped
    direction = first_new / BIAS_ONE / (jnp.sqrt(second_new / BIAS_TWO) + ADAM_EPS) + DECAY * master
    layer_rate = layer_rates[:, None, None, None]
    master_new = master - layer_rate * direction
    teacher_new = EMA_KEEP * teacher + (1.0 - EMA_KEEP) * master_new
    both = jnp.concatenate([master_new.astype(BF16), teacher_new.astype(BF16)], axis=0).reshape(48, 4, 256)
    pieces = place(gather_z(both), [(z + j) & 7 for j in range(8)]).reshape(48, 32, 256)
    students, teachers = gather_x(pieces[:24], pieces[24:])
    at = [((x + j) & 3) * 2 for j in range(4)]
    at = [i + c for i in at] + [i + 1 - c for i in at]
    student = place(students + [shift(s, "c", 1) for s in students], at).reshape(12, 2, 256, 256)
    teach = place(teachers + [shift(t, "c", 1) for t in teachers], at).reshape(12, 2, 256, 256)
    return (master_new, teacher_new, first_new, second_new, student, teach)


def solution(mesh):
    torus = Mesh(mesh.devices.reshape(4, 2, 8, 4), ("x", "c", "z", "y"))
    own = P(None, None, OWN, "y")
    gathered = P(None, None, None, "y")
    in_specs = (P(OWN, None, None, None, "y"), own, own, own, own, P())
    out_specs = (own, own, own, own, gathered, gathered)
    return jax.shard_map(shards, mesh=torus, in_specs=in_specs, out_specs=out_specs, check_vma=False)
```
